32 devices in a mesh: wide: 16 (over z, x, core), narrow: 2 (over y).
Axes of the slice: x: 2, y: 2, z: 4, core: 2. Of those that a mesh axis runs over, the one named last changes fastest.
Arguments:
- vectors: float32 [1024, 16384], P('narrow', 'wide'), may hold values from -6 to 6
- weights: bfloat16 [5, 64, 256, 512], P(None, 'wide', 'narrow'), may hold values from -0.25 to 0.25
Outputs:
- transformed: float32 [1024, 16384], P('narrow', 'wide')
The draws below stay inside these ranges and needn't reach their ends.
All inputs are finite; a program needn't handle non-finite values.
Results may differ from the reference program's by a relative error of at most 0.0003.
Values may be sent and summed in bfloat16 or wider, within the bound.
A program may use at most 64 MiB of HBM per device.

```python
import jax
import jax.numpy as jnp
from jax import lax

BLK_DEV = 4
BLOCK = 256
LEVELS = 5
VECTORS = 1024
BLOCKS = 64
COEFFS = 16384
N_WIDE = 16


def steps_of(key, shape, shards, low, top_value):
    gain, own = 1.0, jax.random.fold_in(key, 6)
    for position, shards_of in shards:
        steps = jnp.exp(jax.random.uniform(jax.random.fold_in(own, position), (shards_of,), jnp.float32, low / len(shards), top_value / len(shards)))
        gain = gain * jnp.repeat(steps, shape[position] // shards_of).reshape([-1 if axis == position else 1 for axis in range(len(shape))])
    return gain


def noise(stream_key, dims, spread, limit, shards=(), dtype=jnp.bfloat16):
    level = steps_of(stream_key, dims, shards, -0.22, 0.18) if shards else 1.0
    array = jax.random.normal(stream_key, dims, jnp.float32) * spread * level
    return jnp.minimum(jnp.maximum(array, -limit), limit).astype(dtype)


def setup_inputs(seed: int = 0) -> dict:
    arg_keys = jax.random.split(jax.random.key(seed), 3)
    vectors = noise(arg_keys[0], (VECTORS, COEFFS), 1.0, 6.0, ((0, 2), (1, 16)), jnp.float32)
    weights = noise(arg_keys[1], (LEVELS, BLOCKS, BLOCK, 2 * BLOCK), (2 * BLOCK) ** -0.5, 0.25, ((1, 16), (2, 2)))
    return dict(vectors=vectors, weights=weights)


def apply_level(current, matrices, level_bit):
    columns, block_count, block_size = current.shape
    stride = 1 << level_bit
    grouped = current.reshape(columns, block_count // (2 * stride), 2, stride, block_size)
    paired = jnp.concatenate([grouped[:, :, 0], grouped[:, :, 1]], -1)
    matrix = matrices.astype(jnp.float32).reshape(block_count // (2 * stride), 2, stride, block_size, 2 * block_size)
    result = jnp.einsum('vaji,asjoi->vasjo', paired, matrix, precision=lax.Precision.HIGHEST)
    return result.reshape(columns, block_count, block_size)


def reference(vectors, weights):
    local_bits = BLK_DEV.bit_length() - 1
    wide_top = N_WIDE.bit_length() - 1
    level_bits = [0, 1, local_bits, local_bits + wide_top // 2, local_bits + wide_top - 1]
    block_size = weights.shape[2]
    current = vectors.reshape(vectors.shape[0], vectors.shape[1] // block_size, block_size)
    for level_index in range(LEVELS):
        current = apply_level(current, weights[level_index], level_bits[level_index])
    return current.reshape(vectors.shape)
```

```python
import functools

import jax
import jax.numpy as jnp
from jax import lax
from jax.experimental import pallas as pl
from jax.experimental.pallas import tpu as pltpu
from jax.sharding import PartitionSpec as P

MESH = pl.DeviceIdType.MESH
POWER = 12
TOP = 2.0 ** (126 / POWER)
TINY = 1e-35
TILE = 128
LOCAL_TILE = 256
WINDOW = 8
BF16 = jnp.bfloat16
F32 = jnp.float32

WEIGHT_ORDER = (
    (0, 0), (0, 2), (1, 0), (2, 0), (3, 0), (1, 2), (2, 2), (0, 1), (3, 2), (0, 3),
    (1, 1), (2, 1), (3, 1), (1, 3), (2, 3), (3, 3), (4, 0), (4, 2), (4, 1), (4, 3),
)
STEPS = (
    ("run", 0, 0, 0, 4), ("run", 0, 2, 0, 4), ("run", 1, 0, 0, 4), ("run", 2, 0, 0, 4),
    ("run", 3, 0, 0, 2), ("run", 1, 2, 0, 4), ("hold", 3, 0, 2, 4), ("run", 2, 2, 0, 4),
    ("send", 3, 0, 2, 4), ("run", 0, 1, 0, 4), ("run", 3, 2, 0, 2), ("run", 0, 3, 0, 4),
    ("hold", 3, 2, 2, 4), ("run", 1, 1, 0, 4), ("run", 2, 1, 0, 4), ("send", 3, 2, 2, 4),
    ("run", 3, 1, 0, 2), ("run", 1, 3, 0, 4), ("hold", 3, 1, 2, 4), ("run", 2, 3, 0, 4),
    ("send", 3, 1, 2, 4), ("run", 3, 3, 0, 4), ("run", 4, 0, 0, 4), ("run", 4, 2, 0, 4),
    ("run", 4, 1, 0, 4), ("run", 4, 3, 0, 4),
)


def split(value):
    high = value.astype(BF16)
    return high, (value - high.astype(F32)).astype(BF16)


def encode(value):
    scale = jnp.maximum(jnp.max(jnp.abs(value), axis=0, keepdims=True), TINY)
    t = value * (TOP / scale)
    t2 = t * t
    t4 = t2 * t2
    t12 = t4 * t4 * t4
    return jnp.where(t < 0, -t12, t12).astype(BF16), scale


def decode(code, scale):
    wide = code.astype(F32)
    size = jnp.exp(jnp.log(jnp.abs(wide)) * (1.0 / POWER)) * (scale * (1.0 / TOP))
    return jnp.where(wide == 0, 0.0, jnp.where(wide < 0, -size, size))


def kernel(
    peers, strides, x_hbm, w_hbm, out,
    x, w, l0, l1, l1_in, l2, z1_out, z1_in, s1_out, s1_in, l3, z2_out, z2_in, s2_out, s2_in,
    x_sem, own_sem, w_send, w_recv, core_send, core_recv, z_send, z_recv, s_send, s_recv,
):
    columns = x.shape[0]
    size = w.shape[3] // 2
    rows = w_hbm.shape[2]
    blocks = w.shape[1]
    tiles = columns // TILE
    me_n = lax.axis_index("narrow")
    me_w = lax.axis_index("wide")
    sides = [me_w // stride % 2 for stride in strides]
    same_way = sides[1] == sides[2]
    partners = [me_w + (1 - 2 * side) * stride for side, stride in zip(sides, strides)]

    def x_copy(half):
        span = pl.ds(half * 2 * size, 2 * size)
        return pltpu.make_async_copy(x_hbm.at[:, span], x.at[:, span], x_sem.at[half])

    def rows_of(owner):
        return pl.ds(pl.multiple_of(owner * rows, rows), rows)

    def own_copy(level, block):
        return pltpu.make_async_copy(
            w_hbm.at[level, block], w.at[level, block, rows_of(me_n)], own_sem.at[level, block]
        )

    def weight_copy(level, block, k, owner):
        return pltpu.make_async_remote_copy(
            src_ref=w.at[level, block, rows_of(owner)],
            dst_ref=w.at[level, block, rows_of(owner)],
            send_sem=w_send.at[level, block, k - 1],
            recv_sem=w_recv.at[level, block, k - 1],
            device_id={"narrow": lax.rem(me_n + k, peers)},
            device_id_type=MESH,
        )

    def send_weight(position):
        if position < len(WEIGHT_ORDER):
            level, block = WEIGHT_ORDER[position]
            own_copy(level, block).wait()
            for k in range(1, peers):
                weight_copy(level, block, k, me_n).start()

    def core_copy(block, tile):
        return pltpu.make_async_remote_copy(
            src_ref=l1.at[block, :, at_tile(tile)], dst_ref=l1_in.at[block, :, at_tile(tile)],
            send_sem=core_send.at[block, tile], recv_sem=core_recv.at[block, tile],
            device_id={"wide": partners[0]}, device_id_type=MESH,
        )

    def code_copies(level, block, tile):
        source, target = ((z1_out, z1_in), (z2_out, z2_in))[level]
        s_source, s_target = ((s1_out, s1_in), (s2_out, s2_in))[level]
        partner = partners[level + 1]
        return (
            pltpu.make_async_remote_copy(
                src_ref=s_source.at[block, tile], dst_ref=s_target.at[block, tile],
                send_sem=s_send.at[level, block, tile], recv_sem=s_recv.at[level, block, tile],
                device_id={"wide": partner}, device_id_type=MESH,
            ),
            pltpu.make_async_remote_copy(
                src_ref=source.at[block, at_tile(tile)], dst_ref=target.at[block, at_tile(tile)],
                send_sem=z_send.at[level, block, tile], recv_sem=z_recv.at[level, block, tile],
                device_id={"wide": partner}, device_id_type=MESH,
            ),
        )

    def send_codes(level, block, tile):
        for copy in code_copies(level, block, tile):
            copy.start()

    def product(level, block, first, second, side, finish, span, height=TILE):
        def step(tile, carry):
            total = None
            for part, half in ((first, side), (second, 1 - side)):
                start = half * size
                if not isinstance(half, int):
                    start = pl.multiple_of(start, size)
                matrix = w[level, block, :, pl.ds(start, size)]
                lhs = jnp.concatenate(part(tile), axis=0)
                term = lax.dot_general(
                    lhs, matrix, (((1,), (1,)), ((), ())), preferred_element_type=F32
                )
                total = term if total is None else total + term
            finish(tile, total[:height] + total[height:])
            return carry

        lax.fori_loop(*span, step, 0)

    def at_tile(tile, height=TILE):
        return pl.ds(pl.multiple_of(tile * height, height), height)

    def from_x(block):
        return lambda tile: split(x[at_tile(tile, LOCAL_TILE), pl.ds(block * size, size)])

    def from_pair(ref, block, height=TILE):
        return lambda tile: (
            ref[block, 0, at_tile(tile, height)], ref[block, 1, at_tile(tile, height)]
        )

    def from_core(block):
        load = from_pair(l1_in, block)

        def wait_and_load(tile):
            core_copy(block, tile).wait_recv()
            return load(tile)

        return wait_and_load

    def from_code(level, block):
        ref, scales = ((z1_in, s1_in), (z2_in, s2_in))[level]

        def load(tile):
            for copy in code_copies(level, block, tile):
                copy.wait_recv()
            return split(decode(ref[block, at_tile(tile)], scales[block, tile]))

        return load

    def to_pair(ref, block, height=TILE):
        def finish(tile, value):
            high, low = split(value)
            ref[block, 0, at_tile(tile, height)] = high
            ref[block, 1, at_tile(tile, height)] = low

        return finish

    def to_core(block):
        keep = to_pair(l1, block, LOCAL_TILE)
        pieces = LOCAL_TILE // TILE

        def finish(tile, value):
            keep(tile, value)
            for piece in range(pieces):
                core_copy(block, tile * pieces + piece).start()

        return finish

    def to_code(level, block, held):
        keep = to_pair((l2, l3)[level], block)
        code_ref, scale_ref = ((z1_out, s1_out), (z2_out, s2_out))[level]

        def finish(tile, value):
            code, scale = encode(value)
            code_ref[block, at_tile(tile)] = code
            scale_ref[block, tile] = scale
            if held:
                pl.when(jnp.logical_not(same_way))(lambda: send_codes(level, block, tile))
            else:
                send_codes(level, block, tile)
            keep(tile, value)

        return finish

    def to_out(block):
        def finish(tile, value):
            out[at_tile(tile), pl.ds(block * size, size)] = value

        return finish

    x_copy(0).start()
    for level, block in WEIGHT_ORDER[:WINDOW]:
        own_copy(level, block).start()
    for half in range(1, blocks // 2):
        x_copy(half).start()
    for level, block in WEIGHT_ORDER[WINDOW:]:
        own_copy(level, block).start()

    barrier = pltpu.get_barrier_semaphore()
    for k in range(1, peers):
        pl.semaphore_signal(
            barrier, inc=1, device_id={"narrow": lax.rem(me_n + k, peers)}, device_id_type=MESH
        )
    for partner in partners:
        pl.semaphore_signal(barrier, inc=1, device_id={"wide": partner}, device_id_type=MESH)
    pl.semaphore_wait(barrier, peers - 1 + len(partners))

    for position in range(WINDOW):
        send_weight(position)

    arrived = [0]

    def need_weight(level, block):
        while (level, block) in WEIGHT_ORDER[arrived[0]:]:
            next_level, next_block = WEIGHT_ORDER[arrived[0]]
            for k in range(1, peers):
                weight_copy(
                    next_level, next_block, k, lax.rem(me_n + peers - k, peers)
                ).wait_recv()
            send_weight(arrived[0] + WINDOW)
            arrived[0] += 1

    x_ready = set()
    local = (0, columns // LOCAL_TILE)
    share = tiles // 4
    for kind, level, block, start, stop in STEPS:
        span = (start * share, stop * share)
        if kind == "send":
            @pl.when(same_way)
            def _():
                def send(tile, carry):
                    send_codes(level - 2, block, tile)
                    return carry

                lax.fori_loop(*span, send, 0)

            continue
        if level == 0 and block // 2 not in x_ready:
            x_copy(block // 2).wait()
            x_ready.add(block // 2)
        need_weight(level, block)
        if level < 2:
            stride = 1 << level
            low = block - block // stride % 2 * stride
            high = low + stride
        if level == 0:
            product(
                level, block, from_x(low), from_x(high), 0, to_pair(l0, block, LOCAL_TILE),
                local, LOCAL_TILE,
            )
        elif level == 1:
            product(
                level, block, from_pair(l0, low, LOCAL_TILE), from_pair(l0, high, LOCAL_TILE), 0,
                to_core(block), local, LOCAL_TILE,
            )
        elif level == 2:
            product(
                level, block, from_pair(l1, block), from_core(block), sides[0],
                to_code(0, block, kind == "hold"), span,
            )
        elif level == 3:
            product(
                level, block, from_pair(l2, block), from_code(0, block), sides[1],
                to_code(1, block, kind == "hold"), span,
            )
        else:
            product(
                level, block, from_pair(l3, block), from_code(1, block), sides[2],
                to_out(block), span,
            )

    for level, block in WEIGHT_ORDER:
        for k in range(1, peers):
            weight_copy(level, block, k, me_n).wait_send()
    for block in range(blocks):
        for tile in range(tiles):
            core_copy(block, tile).wait_send()
            for level in range(2):
                for copy in code_copies(level, block, tile):
                    copy.wait_send()


def on_device(vectors, weights):
    columns, coeffs = vectors.shape
    levels, blocks, rows, depth = weights.shape
    size = depth // 2
    peers = lax.axis_size("narrow")
    wide_top = lax.axis_size("wide").bit_length() - 1
    strides = [1 << bit for bit in (0, wide_top // 2, wide_top - 1)]
    tiles = columns // TILE
    pair = pltpu.VMEM((blocks, 2, columns, size), BF16)
    code = pltpu.VMEM((blocks, columns, size), BF16)
    scale = pltpu.VMEM((blocks, tiles, 1, size), F32)
    dma = pltpu.SemaphoreType.DMA
    return pl.pallas_call(
        functools.partial(kernel, peers, strides),
        out_shape=pltpu.VMEM((columns, coeffs), F32),
        in_specs=[pl.BlockSpec(memory_space=pltpu.HBM)] * 2,
        out_specs=pl.BlockSpec(memory_space=pltpu.VMEM),
        scratch_shapes=[
            pltpu.VMEM((columns, coeffs), F32),
            pltpu.VMEM((levels, blocks, size, depth), BF16),
            pair, pair, pair, pair,
            code, code, scale, scale,
            pair,
            code, code, scale, scale,
            dma((blocks // 2,)),
            dma((levels, blocks)),
            dma((levels, blocks, max(peers - 1, 1))),
            dma((levels, blocks, max(peers - 1, 1))),
            dma((blocks, tiles)),
            dma((blocks, tiles)),
            dma((2, blocks, tiles)),
            dma((2, blocks, tiles)),
            dma((2, blocks, tiles)),
            dma((2, blocks, tiles)),
        ],
        compiler_params=pltpu.CompilerParams(
            collective_id=0, has_side_effects=True, vmem_limit_bytes=61 * 1024 * 1024
        ),
    )(vectors, weights)


def solution(mesh):
    placed = (P("narrow", "wide"), P(None, "wide", "narrow", None))
    return jax.shard_map(
        on_device, mesh=mesh, in_specs=placed, out_specs=P("narrow", "wide"), check_vma=False
    )
```

```python
import functools

import jax
import jax.numpy as jnp
from jax import lax
from jax.experimental import pallas as pl
from jax.experimental.pallas import tpu as pltpu
from jax.sharding import PartitionSpec as P

MESH = pl.DeviceIdType.MESH
POWER = 12
TOP = 2.0 ** (126 / POWER)
TINY = 1e-35
TILE = 128
LOCAL_TILE = 256
WINDOW = 8
BF16 = jnp.bfloat16
F32 = jnp.float32

WEIGHT_ORDER = (
    (0, 0), (0, 2), (1, 0), (2, 0), (3, 0), (1, 2), (2, 2), (0, 1), (3, 2), (0, 3),
    (1, 1), (2, 1), (3, 1), (1, 3), (2, 3), (4, 0), (3, 3), (4, 2), (4, 1), (4, 3),
)
STEPS = (
    ("run", 0, 0, 0, 4), ("run", 0, 2, 0, 4), ("run", 1, 0, 0, 4), ("run", 2, 0, 0, 4),
    ("run", 3, 0, 0, 2), ("run", 1, 2, 0, 4), ("hold", 3, 0, 2, 4), ("run", 2, 2, 0, 4),
    ("send", 3, 0, 2, 4), ("run", 0, 1, 0, 4), ("run", 3, 2, 0, 2), ("run", 0, 3, 0, 4),
    ("run", 1, 1, 0, 4), ("run", 3, 2, 2, 4), ("run", 2, 1, 0, 4), ("run", 1, 3, 0, 4),
    ("run", 3, 1, 0, 2), ("run", 2, 3, 0, 4), ("run", 3, 1, 2, 4), ("run", 3, 3, 0, 2),
    ("run", 4, 0, 0, 4), ("run", 4, 2, 0, 4), ("run", 3, 3, 2, 4), ("drain", 0, 0, 0, 4),
    ("run", 4, 1, 0, 4), ("run", 4, 3, 0, 4),
)


def split(value):
    high = value.astype(BF16)
    return high, (value - high.astype(F32)).astype(BF16)


def encode(value):
    scale = jnp.maximum(jnp.max(jnp.abs(value), axis=0, keepdims=True), TINY)
    t = value * (TOP / scale)
    t2 = t * t
    t4 = t2 * t2
    t12 = t4 * t4 * t4
    return jnp.where(t < 0, -t12, t12).astype(BF16), scale


def decode(code, scale):
    wide = code.astype(F32)
    size = jnp.exp(jnp.log(jnp.abs(wide)) * (1.0 / POWER)) * (scale * (1.0 / TOP))
    return jnp.where(wide == 0, 0.0, jnp.where(wide < 0, -size, size))


def kernel(
    peers, strides, x_hbm, w_hbm, out,
    x, w, l0, l1, l1_in, l2, z1_out, z1_in, s1_out, s1_in, l3, z2_out, z2_in, s2_out, s2_in,
    x_sem, own_sem, w_send, w_recv, core_send, core_recv, z_send, z_recv, s_send, s_recv,
):
    columns = x.shape[0]
    size = w.shape[3] // 2
    rows = w_hbm.shape[2]
    blocks = w.shape[1]
    tiles = columns // TILE
    me_n = lax.axis_index("narrow")
    me_w = lax.axis_index("wide")
    sides = [me_w // stride % 2 for stride in strides]
    same_way = sides[1] == sides[2]
    partners = [me_w + (1 - 2 * side) * stride for side, stride in zip(sides, strides)]

    def x_copy(half):
        span = pl.ds(half * 2 * size, 2 * size)
        return pltpu.make_async_copy(x_hbm.at[:, span], x.at[:, span], x_sem.at[half])

    def rows_of(owner):
        return pl.ds(pl.multiple_of(owner * rows, rows), rows)

    def own_copy(level, block):
        return pltpu.make_async_copy(
            w_hbm.at[level, block], w.at[level, block, rows_of(me_n)], own_sem.at[level, block]
        )

    def weight_copy(level, block, k, owner):
        return pltpu.make_async_remote_copy(
            src_ref=w.at[level, block, rows_of(owner)],
            dst_ref=w.at[level, block, rows_of(owner)],
            send_sem=w_send.at[level, block, k - 1],
            recv_sem=w_recv.at[level, block, k - 1],
            device_id={"narrow": lax.rem(me_n + k, peers)},
            device_id_type=MESH,
        )

    def send_weight(position):
        if position < len(WEIGHT_ORDER):
            level, block = WEIGHT_ORDER[position]
            own_copy(level, block).wait()
            for k in range(1, peers):
                weight_copy(level, block, k, me_n).start()

    def core_copy(block, tile):
        return pltpu.make_async_remote_copy(
            src_ref=l1.at[block, :, at_tile(tile)], dst_ref=l1_in.at[block, :, at_tile(tile)],
            send_sem=core_send.at[block, tile], recv_sem=core_recv.at[block, tile],
            device_id={"wide": partners[0]}, device_id_type=MESH,
        )

    def code_copies(level, block, tile):
        source, target = ((z1_out, z1_in), (z2_out, z2_in))[level]
        s_source, s_target = ((s1_out, s1_in), (s2_out, s2_in))[level]
        partner = partners[level + 1]
        return (
            pltpu.make_async_remote_copy(
                src_ref=s_source.at[block, tile], dst_ref=s_target.at[block, tile],
                send_sem=s_send.at[level, block, tile], recv_sem=s_recv.at[level, block, tile],
                device_id={"wide": partner}, device_id_type=MESH,
            ),
            pltpu.make_async_remote_copy(
                src_ref=source.at[block, at_tile(tile)], dst_ref=target.at[block, at_tile(tile)],
                send_sem=z_send.at[level, block, tile], recv_sem=z_recv.at[level, block, tile],
                device_id={"wide": partner}, device_id_type=MESH,
            ),
        )

    def send_codes(level, block, tile):
        for copy in code_copies(level, block, tile):
            copy.start()

    def product(level, block, first, second, side, finish, span, height=TILE):
        def step(tile, carry):
            total = None
            for part, half in ((first, side), (second, 1 - side)):
                start = half * size
                if not isinstance(half, int):
                    start = pl.multiple_of(start, size)
                matrix = w[level, block, :, pl.ds(start, size)]
                lhs = jnp.concatenate(part(tile), axis=0)
                term = lax.dot_general(
                    lhs, matrix, (((1,), (1,)), ((), ())), preferred_element_type=F32
                )
                total = term if total is None else total + term
            finish(tile, total[:height] + total[height:])
            return carry

        lax.fori_loop(*span, step, 0)

    def at_tile(tile, height=TILE):
        return pl.ds(pl.multiple_of(tile * height, height), height)

    def from_x(block):
        return lambda tile: split(x[at_tile(tile, LOCAL_TILE), pl.ds(block * size, size)])

    def from_pair(ref, block, height=TILE):
        return lambda tile: (
            ref[block, 0, at_tile(tile, height)], ref[block, 1, at_tile(tile, height)]
        )

    def from_core(block):
        load = from_pair(l1_in, block)

        def wait_and_load(tile):
            core_copy(block, tile).wait_recv()
            return load(tile)

        return wait_and_load

    def from_code(level, block):
        ref, scales = ((z1_in, s1_in), (z2_in, s2_in))[level]

        def load(tile):
            for copy in code_copies(level, block, tile):
                copy.wait_recv()
            return split(decode(ref[block, at_tile(tile)], scales[block, tile]))

        return load

    def to_pair(ref, block, height=TILE):
        def finish(tile, value):
            high, low = split(value)
            ref[block, 0, at_tile(tile, height)] = high
            ref[block, 1, at_tile(tile, height)] = low

        return finish

    def to_core(block):
        keep = to_pair(l1, block, LOCAL_TILE)
        pieces = LOCAL_TILE // TILE

        def finish(tile, value):
            keep(tile, value)
            for piece in range(pieces):
                core_copy(block, tile * pieces + piece).start()

        return finish

    def to_code(level, block, kind):
        keep = to_pair((l2, l3)[level], block)
        code_ref, scale_ref = ((z1_out, s1_out), (z2_out, s2_out))[level]

        def finish(tile, value):
            code, scale = encode(value)
            code_ref[block, at_tile(tile)] = code
            scale_ref[block, tile] = scale
            if kind == "hold":
                pl.when(jnp.logical_not(same_way))(lambda: send_codes(level, block, tile))
            elif kind == "holdi":
                pl.when(same_way)(lambda: send_codes(level, block, tile))
            elif kind == "run":
                send_codes(level, block, tile)
            keep(tile, value)

        return finish

    def to_out(block):
        def finish(tile, value):
            out[at_tile(tile), pl.ds(block * size, size)] = value

        return finish

    for position, (level, block) in enumerate(WEIGHT_ORDER):
        own_copy(level, block).start()
        if position in (0, 4):
            for half in range(position // 4, blocks // 2 if position else 1):
                x_copy(half).start()

    barrier = pltpu.get_barrier_semaphore()
    for k in range(1, peers):
        pl.semaphore_signal(
            barrier, inc=1, device_id={"narrow": lax.rem(me_n + k, peers)}, device_id_type=MESH
        )
    for partner in partners:
        pl.semaphore_signal(barrier, inc=1, device_id={"wide": partner}, device_id_type=MESH)
    pl.semaphore_wait(barrier, peers - 1 + len(partners))

    for position in range(WINDOW):
        send_weight(position)

    arrived = [0]

    def need_weight(level, block):
        while (level, block) in WEIGHT_ORDER[arrived[0]:]:
            next_level, next_block = WEIGHT_ORDER[arrived[0]]
            for k in range(1, peers):
                weight_copy(
                    next_level, next_block, k, lax.rem(me_n + peers - k, peers)
                ).wait_recv()
            send_weight(arrived[0] + WINDOW)
            arrived[0] += 1

    x_ready = set()
    local = (0, columns // LOCAL_TILE)
    share = tiles // 4
    for kind, level, block, start, stop in STEPS:
        span = (start * share, stop * share)
        if kind == "drain":
            for level, block in WEIGHT_ORDER:
                for k in range(1, peers):
                    weight_copy(level, block, k, me_n).wait_send()
            for block in range(blocks):
                for tile in range(tiles):
                    core_copy(block, tile).wait_send()
                    for copy in code_copies(0, block, tile):
                        copy.wait_send()
            continue
        if kind.startswith("send"):
            @pl.when({"send": same_way, "sendi": jnp.logical_not(same_way), "senda": True}[kind])
            def _():
                def send(tile, carry):
                    send_codes(level - 2, block, tile)
                    return carry

                lax.fori_loop(*span, send, 0)

            continue
        if level == 0 and block // 2 not in x_ready:
            x_copy(block // 2).wait()
            x_ready.add(block // 2)
        need_weight(level, block)
        if level < 2:
            stride = 1 << level
            low = block - block // stride % 2 * stride
            high = low + stride
        if level == 0:
            product(
                level, block, from_x(low), from_x(high), 0, to_pair(l0, block, LOCAL_TILE),
                local, LOCAL_TILE,
            )
        elif level == 1:
            product(
                level, block, from_pair(l0, low, LOCAL_TILE), from_pair(l0, high, LOCAL_TILE), 0,
                to_core(block), local, LOCAL_TILE,
            )
        elif level == 2:
            product(
                level, block, from_pair(l1, block), from_core(block), sides[0],
                to_code(0, block, kind), span,
            )
        elif level == 3:
            product(
                level, block, from_pair(l2, block), from_code(0, block), sides[1],
                to_code(1, block, kind), span,
            )
        else:
            product(
                level, block, from_pair(l3, block), from_code(1, block), sides[2],
                to_out(block), span,
            )

    for block in range(blocks):
        for tile in range(tiles):
            for copy in code_copies(1, block, tile):
                copy.wait_send()


def on_device(vectors, weights):
    columns, coeffs = vectors.shape
    levels, blocks, rows, depth = weights.shape
    size = depth // 2
    peers = lax.axis_size("narrow")
    wide_top = lax.axis_size("wide").bit_length() - 1
    strides = [1 << bit for bit in (0, wide_top // 2, wide_top - 1)]
    tiles = columns // TILE
    pair = pltpu.VMEM((blocks, 2, columns, size), BF16)
    code = pltpu.VMEM((blocks, columns, size), BF16)
    scale = pltpu.VMEM((blocks, tiles, 1, size), F32)
    dma = pltpu.SemaphoreType.DMA
    return pl.pallas_call(
        functools.partial(kernel, peers, strides),
        out_shape=pltpu.VMEM((columns, coeffs), F32),
        in_specs=[pl.BlockSpec(memory_space=pltpu.HBM)] * 2,
        out_specs=pl.BlockSpec(memory_space=pltpu.VMEM),
        scratch_shapes=[
            pltpu.VMEM((columns, coeffs), F32),
            pltpu.VMEM((levels, blocks, size, depth), BF16),
            pair, pair, pair, pair,
            code, code, scale, scale,
            pair,
            code, code, scale, scale,
            dma((blocks // 2,)),
            dma((levels, blocks)),
            dma((levels, blocks, max(peers - 1, 1))),
            dma((levels, blocks, max(peers - 1, 1))),
            dma((blocks, tiles)),
            dma((blocks, tiles)),
            dma((2, blocks, tiles)),
            dma((2, blocks, tiles)),
            dma((2, blocks, tiles)),
            dma((2, blocks, tiles)),
        ],
        compiler_params=pltpu.CompilerParams(
            collective_id=0, has_side_effects=True, vmem_limit_bytes=61 * 1024 * 1024
        ),
    )(vectors, weights)


def solution(mesh):
    placed = (P("narrow", "wide"), P(None, "wide", "narrow", None))
    return jax.shard_map(
        on_device, mesh=mesh, in_specs=placed, out_specs=P("narrow", "wide"), check_vma=False
    )
```

```python
import functools

import jax
import jax.numpy as jnp
from jax import lax
from jax.experimental import pallas as pl
from jax.experimental.pallas import tpu as pltpu
from jax.sharding import PartitionSpec as P

MESH = pl.DeviceIdType.MESH
POWER = 12
TOP = 2.0 ** (126 / POWER)
TINY = 1e-35
TILE = 128
LOCAL_TILE = 256
WINDOW = 8
BF16 = jnp.bfloat16
F32 = jnp.float32

WEIGHT_ORDER = (
    (0, 0), (0, 2), (1, 0), (2, 0), (3, 0), (1, 2), (2, 2), (0, 1), (3, 2), (0, 3),
    (1, 1), (2, 1), (3, 1), (1, 3), (2, 3), (4, 0), (3, 3), (4, 2), (4, 1), (4, 3),
)
STEPS = (
    ("run", 0, 0, 0, 4), ("run", 0, 2, 0, 4), ("run", 1, 0, 0, 4), ("run", 2, 0, 0, 4),
    ("run", 3, 0, 0, 2), ("run", 1, 2, 0, 4), ("hold", 3, 0, 2, 4), ("run", 2, 2, 0, 4),
    ("send", 3, 0, 2, 4), ("run", 0, 1, 0, 4), ("run", 3, 2, 0, 2), ("run", 0, 3, 0, 4),
    ("run", 1, 1, 0, 4), ("holdi", 3, 2, 2, 3), ("holdi", 3, 2, 3, 4), ("run", 2, 1, 0, 2),
    ("sendi", 3, 2, 2, 3), ("run", 2, 1, 2, 4), ("sendi", 3, 2, 3, 4), ("run", 1, 3, 0, 4),
    ("run", 3, 1, 0, 2), ("run", 2, 3, 0, 4), ("run", 3, 1, 2, 4), ("run", 3, 3, 0, 2),
    ("run", 4, 0, 0, 4), ("run", 4, 2, 0, 4), ("run", 3, 3, 2, 4), ("drain", 0, 0, 0, 4),
    ("tall", 4, 1, 0, 4), ("run", 4, 3, 0, 4),
)


def split(value):
    high = value.astype(BF16)
    return high, (value - high.astype(F32)).astype(BF16)


def encode(value):
    scale = jnp.maximum(jnp.max(jnp.abs(value), axis=0, keepdims=True), TINY)
    t = value * (TOP / scale)
    t2 = t * t
    t4 = t2 * t2
    t12 = t4 * t4 * t4
    return jnp.where(t < 0, -t12, t12).astype(BF16), scale


def decode(code, scale):
    wide = code.astype(F32)
    size = jnp.exp(jnp.log(jnp.abs(wide)) * (1.0 / POWER)) * (scale * (1.0 / TOP))
    return jnp.where(wide == 0, 0.0, jnp.where(wide < 0, -size, size))


def kernel(
    peers, strides, x_hbm, w_hbm, out,
    x, w, l0, l1, l1_in, l2, z1_out, z1_in, s1_out, s1_in, l3, z2_out, z2_in, s2_out, s2_in,
    x_sem, own_sem, w_send, w_recv, core_send, core_recv, z_send, z_recv, s_send, s_recv,
):
    columns = x.shape[0]
    size = w.shape[3] // 2
    rows = w_hbm.shape[2]
    blocks = w.shape[1]
    tiles = columns // TILE
    me_n = lax.axis_index("narrow")
    me_w = lax.axis_index("wide")
    sides = [me_w // stride % 2 for stride in strides]
    same_way = sides[1] == sides[2]
    partners = [me_w + (1 - 2 * side) * stride for side, stride in zip(sides, strides)]

    def x_copy(half):
        span = pl.ds(half * 2 * size, 2 * size)
        return pltpu.make_async_copy(x_hbm.at[:, span], x.at[:, span], x_sem.at[half])

    def rows_of(owner):
        return pl.ds(pl.multiple_of(owner * rows, rows), rows)

    def own_copy(level, block):
        return pltpu.make_async_copy(
            w_hbm.at[level, block], w.at[level, block, rows_of(me_n)], own_sem.at[level, block]
        )

    def weight_copy(level, block, k, owner):
        return pltpu.make_async_remote_copy(
            src_ref=w.at[level, block, rows_of(owner)],
            dst_ref=w.at[level, block, rows_of(owner)],
            send_sem=w_send.at[level, block, k - 1],
            recv_sem=w_recv.at[level, block, k - 1],
            device_id={"narrow": lax.rem(me_n + k, peers)},
            device_id_type=MESH,
        )

    def send_weight(position):
        if position < len(WEIGHT_ORDER):
            level, block = WEIGHT_ORDER[position]
            own_copy(level, block).wait()
            for k in range(1, peers):
                weight_copy(level, block, k, me_n).start()

    def core_copy(block, tile):
        return pltpu.make_async_remote_copy(
            src_ref=l1.at[block, :, at_tile(tile)], dst_ref=l1_in.at[block, :, at_tile(tile)],
            send_sem=core_send.at[block, tile], recv_sem=core_recv.at[block, tile],
            device_id={"wide": partners[0]}, device_id_type=MESH,
        )

    def code_copies(level, block, tile):
        source, target = ((z1_out, z1_in), (z2_out, z2_in))[level]
        s_source, s_target = ((s1_out, s1_in), (s2_out, s2_in))[level]
        partner = partners[level + 1]
        return (
            pltpu.make_async_remote_copy(
                src_ref=s_source.at[block, tile], dst_ref=s_target.at[block, tile],
                send_sem=s_send.at[level, block, tile], recv_sem=s_recv.at[level, block, tile],
                device_id={"wide": partner}, device_id_type=MESH,
            ),
            pltpu.make_async_remote_copy(
                src_ref=source.at[block, at_tile(tile)], dst_ref=target.at[block, at_tile(tile)],
                send_sem=z_send.at[level, block, tile], recv_sem=z_recv.at[level, block, tile],
                device_id={"wide": partner}, device_id_type=MESH,
            ),
        )

    def send_codes(level, block, tile):
        for copy in code_copies(level, block, tile):
            copy.start()

    def product(level, block, first, second, side, finish, span, height=TILE):
        def step(tile, carry):
            total = None
            for part, half in ((first, side), (second, 1 - side)):
                start = half * size
                if not isinstance(half, int):
                    start = pl.multiple_of(start, size)
                matrix = w[level, block, :, pl.ds(start, size)]
                lhs = jnp.concatenate(part(tile), axis=0)
                term = lax.dot_general(
                    lhs, matrix, (((1,), (1,)), ((), ())), preferred_element_type=F32
                )
                total = term if total is None else total + term
            finish(tile, total[:height] + total[height:])
            return carry

        lax.fori_loop(*span, step, 0)

    def at_tile(tile, height=TILE):
        return pl.ds(pl.multiple_of(tile * height, height), height)

    def from_x(block):
        return lambda tile: split(x[at_tile(tile, LOCAL_TILE), pl.ds(block * size, size)])

    def from_pair(ref, block, height=TILE):
        return lambda tile: (
            ref[block, 0, at_tile(tile, height)], ref[block, 1, at_tile(tile, height)]
        )

    def from_core(block):
        load = from_pair(l1_in, block)

        def wait_and_load(tile):
            core_copy(block, tile).wait_recv()
            return load(tile)

        return wait_and_load

    def from_code(level, block):
        ref, scales = ((z1_in, s1_in), (z2_in, s2_in))[level]

        def load(tile):
            for copy in code_copies(level, block, tile):
                copy.wait_recv()
            return split(decode(ref[block, at_tile(tile)], scales[block, tile]))

        return load

    def from_codes(level, block):
        load = from_code(level, block)
        pieces = LOCAL_TILE // TILE

        def load_tall(tile):
            parts = [load(tile * pieces + piece) for piece in range(pieces)]
            return [jnp.concatenate(part, axis=0) for part in zip(*parts)]

        return load_tall

    def to_pair(ref, block, height=TILE):
        def finish(tile, value):
            high, low = split(value)
            ref[block, 0, at_tile(tile, height)] = high
            ref[block, 1, at_tile(tile, height)] = low

        return finish

    def to_core(block):
        keep = to_pair(l1, block, LOCAL_TILE)
        pieces = LOCAL_TILE // TILE

        def finish(tile, value):
            keep(tile, value)
            for piece in range(pieces):
                core_copy(block, tile * pieces + piece).start()

        return finish

    def to_code(level, block, kind):
        keep = to_pair((l2, l3)[level], block)
        code_ref, scale_ref = ((z1_out, s1_out), (z2_out, s2_out))[level]

        def finish(tile, value):
            code, scale = encode(value)
            code_ref[block, at_tile(tile)] = code
            scale_ref[block, tile] = scale
            if kind == "hold":
                pl.when(jnp.logical_not(same_way))(lambda: send_codes(level, block, tile))
            elif kind == "holdi":
                pl.when(same_way)(lambda: send_codes(level, block, tile))
            elif kind == "run":
                send_codes(level, block, tile)
            keep(tile, value)

        return finish

    def to_out(block, height=TILE):
        def finish(tile, value):
            out[at_tile(tile, height), pl.ds(block * size, size)] = value

        return finish

    for position, (level, block) in enumerate(WEIGHT_ORDER):
        own_copy(level, block).start()
        if position in (0, 4):
            for half in range(position // 4, blocks // 2 if position else 1):
                x_copy(half).start()

    barrier = pltpu.get_barrier_semaphore()
    for k in range(1, peers):
        pl.semaphore_signal(
            barrier, inc=1, device_id={"narrow": lax.rem(me_n + k, peers)}, device_id_type=MESH
        )
    for partner in partners:
        pl.semaphore_signal(barrier, inc=1, device_id={"wide": partner}, device_id_type=MESH)
    pl.semaphore_wait(barrier, peers - 1 + len(partners))

    for position in range(WINDOW):
        send_weight(position)

    arrived = [0]

    def need_weight(level, block):
        while (level, block) in WEIGHT_ORDER[arrived[0]:]:
            next_level, next_block = WEIGHT_ORDER[arrived[0]]
            for k in range(1, peers):
                weight_copy(
                    next_level, next_block, k, lax.rem(me_n + peers - k, peers)
                ).wait_recv()
            send_weight(arrived[0] + WINDOW)
            arrived[0] += 1

    x_ready = set()
    local = (0, columns // LOCAL_TILE)
    share = tiles // 4
    for kind, level, block, start, stop in STEPS:
        span = (start * share, stop * share)
        if kind == "drain":
            for level, block in WEIGHT_ORDER:
                for k in range(1, peers):
                    weight_copy(level, block, k, me_n).wait_send()
            for block in range(blocks):
                for tile in range(tiles):
                    core_copy(block, tile).wait_send()
                    for copy in code_copies(0, block, tile):
                        copy.wait_send()
            continue
        if kind.startswith("send"):
            @pl.when({"send": same_way, "sendi": jnp.logical_not(same_way), "senda": True}[kind])
            def _():
                def send(tile, carry):
                    send_codes(level - 2, block, tile)
                    return carry

                lax.fori_loop(*span, send, 0)

            continue
        if level == 0 and block // 2 not in x_ready:
            x_copy(block // 2).wait()
            x_ready.add(block // 2)
        need_weight(level, block)
        if level < 2:
            stride = 1 << level
            low = block - block // stride % 2 * stride
            high = low + stride
        if level == 0:
            product(
                level, block, from_x(low), from_x(high), 0, to_pair(l0, block, LOCAL_TILE),
                local, LOCAL_TILE,
            )
        elif level == 1:
            product(
                level, block, from_pair(l0, low, LOCAL_TILE), from_pair(l0, high, LOCAL_TILE), 0,
                to_core(block), local, LOCAL_TILE,
            )
        elif level == 2:
            product(
                level, block, from_pair(l1, block), from_core(block), sides[0],
                to_code(0, block, kind), span,
            )
        elif level == 3:
            product(
                level, block, from_pair(l2, block), from_code(0, block), sides[1],
                to_code(1, block, kind), span,
            )
        elif kind == "tall":
            product(
                level, block, from_pair(l3, block, LOCAL_TILE), from_codes(1, block), sides[2],
                to_out(block, LOCAL_TILE), local, LOCAL_TILE,
            )
        else:
            product(
                level, block, from_pair(l3, block), from_code(1, block), sides[2],
                to_out(block), span,
            )

    for block in range(blocks):
        for tile in range(tiles):
            for copy in code_copies(1, block, tile):
                copy.wait_send()


def on_device(vectors, weights):
    columns, coeffs = vectors.shape
    levels, blocks, rows, depth = weights.shape
    size = depth // 2
    peers = lax.axis_size("narrow")
    wide_top = lax.axis_size("wide").bit_length() - 1
    strides = [1 << bit for bit in (0, wide_top // 2, wide_top - 1)]
    tiles = columns // TILE
    pair = pltpu.VMEM((blocks, 2, columns, size), BF16)
    code = pltpu.VMEM((blocks, columns, size), BF16)
    scale = pltpu.VMEM((blocks, tiles, 1, size), F32)
    dma = pltpu.SemaphoreType.DMA
    return pl.pallas_call(
        functools.partial(kernel, peers, strides),
        out_shape=pltpu.VMEM((columns, coeffs), F32),
        in_specs=[pl.BlockSpec(memory_space=pltpu.HBM)] * 2,
        out_specs=pl.BlockSpec(memory_space=pltpu.VMEM),
        scratch_shapes=[
            pltpu.VMEM((columns, coeffs), F32),
            pltpu.VMEM((levels, blocks, size, depth), BF16),
            pair, pair, pair, pair,
            code, code, scale, scale,
            pair,
            code, code, scale, scale,
            dma((blocks // 2,)),
            dma((levels, blocks)),
            dma((levels, blocks, max(peers - 1, 1))),
            dma((levels, blocks, max(peers - 1, 1))),
            dma((blocks, tiles)),
            dma((blocks, tiles)),
            dma((2, blocks, tiles)),
            dma((2, blocks, tiles)),
            dma((2, blocks, tiles)),
            dma((2, blocks, tiles)),
        ],
        compiler_params=pltpu.CompilerParams(
            collective_id=0, has_side_effects=True, vmem_limit_bytes=61 * 1024 * 1024
        ),
    )(vectors, weights)


def solution(mesh):
    placed = (P("narrow", "wide"), P(None, "wide", "narrow", None))
    return jax.shard_map(
        on_device, mesh=mesh, in_specs=placed, out_specs=P("narrow", "wide"), check_vma=False
    )
```
